256 devices in a mesh: traj: 16 (over z, core), amp: 16 (over x, y).
Axes of the slice: x: 4, y: 4, z: 8, core: 2. Of those that a mesh axis runs over, the one named last changes fastest.
Arguments:
- amplitudes: float32 [16, 2, 524288], P('traj', None, 'amp'), parts along dimension 0, may hold values from -6 to 6
- couplings: float32 [18], replicated, may hold values from 0.5 to 2
- fields: float32 [19], replicated, may hold values from 0.5 to 2
- decays: float32 [19], replicated, may hold values from 0.2 to 2
- channel: int32 [16], P('traj'), parts along dimension 0, may hold values from 0 to 19
Outputs:
- evolved_state: float32 [16, 2, 524288], P('traj', None, 'amp'), parts along dimension 0
The draws below stay inside these ranges and needn't reach their ends.
There are 16 independent parts, one for each index of `traj`. The reference program is written for one: setup_inputs(seed, part) draws one part's arguments, and reference() takes and returns one part's arrays. A program takes and returns all parts, laid end to end along the dimension named above; an argument that names none is the same for every part. Nothing has to cross between parts.
Inputs may be any that keep to these rules, and one draw needn't show every extreme that they name: `channel`: the value 19 means that the trajectory does not jump.
All inputs are finite; a program needn't handle non-finite values.
Results may differ from the reference program's by a relative error of at most 0.0003.
Values sent between devices are 32-bit elements; how exact they have to be, the bound alone decides.
A program may use at most 128 MiB of HBM per device.

```python
import math
import jax
import jax.numpy as jnp
from jax import lax

SPINS = 19
KRYLOV = 8
TRAJ = 1
AMPS = 524288


def steps_of(rng, dims, cuts, smallest, largest):
    def one(dim, shards_of):
        steps = jax.random.uniform(jax.random.fold_in(jax.random.fold_in(rng, 6), dim), (shards_of,), jnp.float32, smallest / len(cuts), largest / len(cuts))
        return jnp.repeat(jnp.exp(steps), dims[dim] // shards_of).reshape((-1,) + (1,) * (len(dims) - dim - 1))

    factor_of = one(*cuts[0])
    for cut in cuts[1:]:
        factor_of = factor_of * one(*cut)
    return factor_of


def noise(stream_key, dims, deviation, most, pieces=(), kind=jnp.bfloat16):
    drawn = jax.random.normal(stream_key, dims, jnp.float32) * deviation
    if len(pieces) > 0:
        drawn = steps_of(stream_key, dims, pieces, -0.22, 0.18) * drawn
    return jnp.clip(drawn, min=-most, max=most).astype(kind)


def setup_inputs(seed: int = 0, part: int = 0) -> dict:
    streams_of = jax.random.split(jax.random.key(seed), 6)
    own_keys = jax.random.split(jax.random.fold_in(streams_of[5], part), 6)
    amplitudes = noise(own_keys[0], (TRAJ, 2, AMPS), 1.0, 6.0, ((2, 16),), jnp.float32)
    couplings = jnp.clip(jnp.exp(jax.random.uniform(streams_of[1], (SPINS - 1,), jnp.float32, math.log(0.5), math.log(2.0))), 0.5, 2.0)
    fields = jnp.clip(jnp.exp(jax.random.uniform(streams_of[2], (SPINS,), jnp.float32, math.log(0.5), math.log(2.0))), 0.5, 2.0)
    decays = jnp.clip(jnp.exp(jax.random.uniform(streams_of[3], (SPINS,), jnp.float32, math.log(0.2), math.log(2.0))), 0.2, 2.0)
    channel = jax.random.randint(own_keys[4], (TRAJ,), 0, SPINS + 1).astype(jnp.int32)
    return dict(amplitudes=amplitudes, couplings=couplings, fields=fields, decays=decays, channel=channel)


time_step = 0.7
squarings = 8
taylor_order = 10
highest = lax.Precision.HIGHEST

def flip_spin(vector, spin_pos):
    leading = vector.shape[:-1]
    length = vector.shape[-1]
    parted = vector.reshape(leading + (length >> spin_pos + 1, 2, 1 << spin_pos))
    return jnp.flip(parted, axis=len(leading) + 1).reshape(vector.shape)

def apply_heff(vector, fields, diag_real, diag_imag):
    flipped = jnp.zeros_like(vector)
    for spin_pos in range(SPINS):
        flipped = flipped + fields[spin_pos] * flip_spin(vector, spin_pos)
    real_part = vector[:, 0]
    imag_part = vector[:, 1]
    out_real = diag_real * real_part - diag_imag * imag_part - flipped[:, 0]
    out_imag = diag_real * imag_part + diag_imag * real_part - flipped[:, 1]
    return jnp.stack([out_real, out_imag], axis=1)

def krylov_weights(scale_norm, hess_real, hess_imag):
    a_real = time_step * hess_imag
    a_imag = -time_step * hess_real
    upper_half = jnp.concatenate([a_real, -a_imag], axis=2)
    lower_half = jnp.concatenate([a_imag, a_real], axis=2)
    scaled = jnp.concatenate([upper_half, lower_half], axis=1) / 2.0 ** squarings
    identity = jnp.broadcast_to(jnp.eye(2 * KRYLOV, dtype=jnp.float32), scaled.shape)
    series = identity
    for degree in range(taylor_order, 0, -1):
        series = identity + jnp.einsum('tij,tjk->tik', scaled, series, precision=highest) / degree
    for repeat in range(squarings):
        series = jnp.einsum('tij,tjk->tik', series, series, precision=highest)
    first_column = series[:, :, 0] * scale_norm[:, None]
    return (first_column[:, :KRYLOV], first_column[:, KRYLOV:])

def reference(amplitudes, couplings, fields, decays, channel):
    traj_count = amplitudes.shape[0]
    position = jnp.arange(AMPS, dtype=jnp.int32)
    occupation = [(position >> spin_pos & 1).astype(jnp.float32) for spin_pos in range(SPINS)]
    diag_real = jnp.zeros((AMPS,), jnp.float32)
    for spin_pos in range(SPINS - 1):
        diag_real = diag_real - couplings[spin_pos] * (1.0 - 2.0 * occupation[spin_pos]) * (1.0 - 2.0 * occupation[spin_pos + 1])
    diag_imag = jnp.zeros((AMPS,), jnp.float32)
    for spin_pos in range(SPINS):
        diag_imag = diag_imag - 0.5 * decays[spin_pos] * occupation[spin_pos]
    scale_norm = jnp.sqrt(lax.optimization_barrier(jnp.sum(amplitudes * amplitudes, axis=(1, 2))))
    krylov_basis = [amplitudes / scale_norm[:, None, None]]
    hess_real = jnp.zeros((traj_count, KRYLOV, KRYLOV), jnp.float32)
    hess_imag = jnp.zeros((traj_count, KRYLOV, KRYLOV), jnp.float32)
    for column in range(KRYLOV):
        applied = apply_heff(krylov_basis[column], fields, diag_real, diag_imag)
        stacked = jnp.stack(krylov_basis, axis=1)
        swapped = jnp.stack([applied[:, 1], -applied[:, 0]], axis=1)
        proj_real = jnp.einsum('tkca,tca->tk', stacked, applied, precision=highest)
        proj_imag = jnp.einsum('tkca,tca->tk', stacked, swapped, precision=highest)
        hess_real = hess_real.at[:, :column + 1, column].set(proj_real)
        hess_imag = hess_imag.at[:, :column + 1, column].set(proj_imag)
        if column + 1 < KRYLOV:
            comb_real = jnp.einsum('tk,tka->ta', proj_real, stacked[:, :, 0], precision=highest) - jnp.einsum('tk,tka->ta', proj_imag, stacked[:, :, 1], precision=highest)
            comb_imag = jnp.einsum('tk,tka->ta', proj_real, stacked[:, :, 1], precision=highest) + jnp.einsum('tk,tka->ta', proj_imag, stacked[:, :, 0], precision=highest)
            residual = applied - jnp.stack([comb_real, comb_imag], axis=1)
            column_norm = jnp.sqrt(lax.optimization_barrier(jnp.sum(residual * residual, axis=(1, 2))))
            hess_real = hess_real.at[:, column + 1, column].set(column_norm)
            krylov_basis.append(residual / column_norm[:, None, None])
    weights_real, weights_imag = krylov_weights(scale_norm, hess_real, hess_imag)
    stacked = jnp.stack(krylov_basis, axis=1)
    new_real = jnp.einsum('tk,tka->ta', weights_real, stacked[:, :, 0], precision=highest) - jnp.einsum('tk,tka->ta', weights_imag, stacked[:, :, 1], precision=highest)
    new_imag = jnp.einsum('tk,tka->ta', weights_real, stacked[:, :, 1], precision=highest) + jnp.einsum('tk,tka->ta', weights_imag, stacked[:, :, 0], precision=highest)
    propagated = jnp.stack([new_real, new_imag], axis=1)
    lowered = jnp.zeros_like(propagated)
    for spin_pos in range(SPINS):
        vacant = occupation[spin_pos] == 0.0
        lowered_term = jnp.where(vacant[None, None, :], flip_spin(propagated, spin_pos), 0.0)
        lowered = jnp.where((channel == spin_pos)[:, None, None], lowered_term, lowered)
    jumped = channel < SPINS
    squared_sum = jnp.where(jumped, lax.optimization_barrier(jnp.sum(lowered * lowered, axis=(1, 2))), jnp.float32(AMPS))
    lowered = lowered * jnp.sqrt(AMPS / squared_sum)[:, None, None]
    return jnp.where(jumped[:, None, None], lowered, propagated)
```

```python
import functools

import jax
import jax.numpy as jnp
from jax import lax
from jax.experimental import pallas as pl
from jax.experimental.pallas import tpu as pltpu
from jax.sharding import PartitionSpec as P

SPINS = 19
KRYLOV = 8
TILES = 32
CHUNKS = 8
PER = TILES // CHUNKS
CHUNK_BITS = CHUNKS.bit_length() - 1
EARLY = 2
TIME_STEP = 0.7
MESH = pl.DeviceIdType.MESH
OWN, DIR_Y, DIR_X, REL_Y, REL_X = range(5)
highest = lax.Precision.HIGHEST
f32 = jnp.float32


def flip(index, bit):
    step = 1 << bit
    return index + step - 2 * step * ((index // step) % 2)


def flip_by(index, mask):
    for bit in range(4):
        if mask >> bit & 1:
            index = flip(index, bit)
    return index


def wide(value):
    return jnp.broadcast_to(value, (8, 128))


def cmul(ar, ai, br, bi):
    return ar * br - ai * bi, ar * bi + ai * br


def matmul8(ar, ai, br, bi):
    out_r, out_i = None, None
    for k in range(KRYLOV):
        cr, ci = ar[:, k : k + 1], ai[:, k : k + 1]
        rr, ri = br[k : k + 1, :], bi[k : k + 1, :]
        tr, ti = cr * rr - ci * ri, cr * ri + ci * rr
        out_r = tr if out_r is None else out_r + tr
        out_i = ti if out_i is None else out_i + ti
    return out_r, out_i


def kernel(
    amp_ref, coup, field, decay, chan, out_ref,
    big, vbuf, zbuf, hbuf, diag_r, diag_i, mask_ref, lanes_ref, acc, total_ref, gather, prop,
    recv_sem, send_sem, red_recv, red_send,
):
    me = lax.axis_index("amp")
    y, x = me % 4, me // 4
    near_y, near_x = x * 4 + flip(y, 0), flip(x, 0) * 4 + y
    far_y, far_x = x * 4 + 3 - y, (3 - x) * 4 + y

    barrier = pltpu.get_barrier_semaphore()
    for mask in range(1, 16):
        pl.semaphore_signal(barrier, inc=1, device_id={"amp": flip_by(me, mask)}, device_id_type=MESH)

    lane = lax.broadcasted_iota(jnp.int32, (8, 128), 1)
    sub = lax.broadcasted_iota(jnp.int32, (8, 128), 0)
    low = sub * 128 + lane

    def direct(step, chunk):
        made = []
        for kind, target in ((DIR_Y, near_y), (DIR_X, near_x)):
            made.append(pltpu.make_async_remote_copy(
                src_ref=big.at[OWN, step, chunk], dst_ref=big.at[kind, step, chunk],
                send_sem=send_sem.at[kind - 1, step], recv_sem=recv_sem.at[kind - 1, step, chunk],
                device_id={"amp": target}, device_id_type=MESH))
        return made

    def relay(step, chunk):
        made = []
        for kind, source, target in ((REL_Y, DIR_Y, far_y), (REL_X, DIR_X, far_x)):
            made.append(pltpu.make_async_remote_copy(
                src_ref=big.at[source, step, chunk], dst_ref=big.at[kind, step, chunk],
                send_sem=send_sem.at[kind - 1, step], recv_sem=recv_sem.at[kind - 1, step, chunk],
                device_id={"amp": target}, device_id_type=MESH))
        return made

    def sum_copy(number, mask):
        return pltpu.make_async_remote_copy(
            src_ref=total_ref.at[number], dst_ref=gather.at[number, mask - 1],
            send_sem=red_send.at[number], recv_sem=red_recv.at[number],
            device_id={"amp": flip_by(me, mask)}, device_id_type=MESH)

    def post_sums(number):
        rows = lax.broadcasted_iota(jnp.int32, (40, 128), 0)
        cols = lax.broadcasted_iota(jnp.int32, (40, 128), 1)
        by_lane = jnp.sum(acc[...], axis=1)
        by_row = jnp.sum(by_lane, axis=1, keepdims=True)
        total_ref[number] = jnp.sum(jnp.where(rows == cols, by_row, 0.0), axis=0, keepdims=True)
        for mask in range(1, 16):
            sum_copy(number, mask).start()

    def take_sums(number):
        pltpu.make_async_copy(gather.at[number], gather.at[number], red_recv.at[number]).wait()
        terms = [total_ref[number]] + [gather[number, i] for i in range(15)]
        while len(terms) > 1:
            terms = [terms[i] + terms[i + 1] for i in range(0, len(terms), 2)]
        return wide(terms[0])

    def pick(row, at):
        return wide(jnp.sum(jnp.where(lane == at, row, 0.0), axis=1, keepdims=True))

    z = [1.0 - 2.0 * (low >> i & 1).astype(f32) for i in range(10)]
    base_r = jnp.zeros((8, 128), f32)
    base_i = jnp.zeros((8, 128), f32)
    for i in range(9):
        base_r = base_r - coup[i] * (z[i] * z[i + 1])
    for i in range(10):
        base_i = base_i - (0.25 * decay[i]) * (1.0 - z[i])
    zdev = [(1 - 2 * ((me // (1 << b)) % 2)).astype(f32) for b in range(4)]
    dev_r = -(coup[15] * zdev[0] * zdev[1] + coup[16] * zdev[1] * zdev[2] + coup[17] * zdev[2] * zdev[3])
    dev_i = jnp.float32(0.0)
    for b in range(4):
        dev_i = dev_i - 0.25 * decay[15 + b] * (1.0 - zdev[b])
    bond = coup[9] * z[9]
    channel = chan[0]
    for tile in range(TILES):
        zt = [1.0 - 2.0 * (tile >> b & 1) for b in range(5)]
        sr, si = dev_r - coup[14] * zdev[0] * zt[4], dev_i
        for b in range(4):
            sr = sr - coup[10 + b] * (zt[b] * zt[b + 1])
        for b in range(5):
            if tile >> b & 1:
                si = si - 0.5 * decay[10 + b]
        diag_r[tile // PER, tile % PER] = (base_r - bond * zt[0]) + sr
        diag_i[tile // PER, tile % PER] = base_i + si
        spot = low + (tile * 1024 + me * 32768)
        mask_ref[tile // PER, tile % PER] = (spot >> jnp.full((8, 128), channel, jnp.int32) & 1).astype(f32)
    li = lax.broadcasted_iota(jnp.int32, (128, 128), 0)
    lj = lax.broadcasted_iota(jnp.int32, (128, 128), 1)
    table = jnp.zeros((128, 128), f32)
    for i in range(7):
        table = table + jnp.where((li ^ lj) == 1 << i, field[i], 0.0)
    lanes_ref[...] = table
    for part in range(2):
        for chunk in range(CHUNKS):
            big[OWN, 0, chunk, part] = amp_ref[part, chunk * PER : (chunk + 1) * PER]
    acc[...] = jnp.zeros((40, 8, 128), f32)

    def local_part(step, chunk):
        v = big[OWN, step, chunk]
        flips = lax.dot_general(
            v.reshape(2 * PER * 8, 128), lanes_ref[...], (((1,), (0,)), ((), ())),
            precision=highest, preferred_element_type=f32).reshape(2 * PER, 8, 128)
        w = v.reshape(2 * PER, 8, 128)
        s3 = lax.broadcasted_iota(jnp.int32, (2 * PER, 8, 128), 1)
        for b in range(2):
            step_rows = 1 << b
            up = pltpu.roll(w, 8 - step_rows, 1)
            down = pltpu.roll(w, step_rows, 1)
            flips = flips + field[7 + b] * jnp.where((s3 >> b & 1) == 0, up, down)
        flips = flips + field[9] * pltpu.roll(w, 4, 1)
        flips = flips.reshape(2, PER, 8, 128)
        for b in range(5 - CHUNK_BITS):
            order = [t ^ (1 << b) for t in range(PER)]
            flips = flips + field[10 + b] * jnp.concatenate([v[:, t : t + 1] for t in order], axis=1)
        for b in range(CHUNK_BITS):
            flips = flips + field[15 - CHUNK_BITS + b] * big[OWN, step, flip(chunk, b)]
        dr, di = diag_r[chunk], diag_i[chunk]
        hr = dr * v[0] - di * v[1] - flips[0]
        hi = dr * v[1] + di * v[0] - flips[1]
        return v, hr, hi

    pl.semaphore_wait(barrier, 15)

    def send_first(chunk, carry):
        for copy in direct(0, chunk):
            copy.start()
        return carry

    lax.fori_loop(0, CHUNKS, send_first, 0)

    def first(chunk, carry):
        v, hr, hi = local_part(0, chunk)
        hbuf[chunk, 0] = hr
        hbuf[chunk, 1] = hi
        acc[0] += jnp.sum(v[0] * hr + v[1] * hi, axis=0)
        acc[8] += jnp.sum(v[0] * hi - v[1] * hr, axis=0)
        acc[32] += jnp.sum(v[0] * v[0] + v[1] * v[1], axis=0)
        return carry

    lax.fori_loop(0, CHUNKS, first, 0)
    post_sums(0)

    zero = jnp.zeros((8, 128), f32)
    hess_r, hess_i = zero, zero
    basis_r, basis_i = zero, zero
    proj_r, proj_i = zero, zero
    shift_r, shift_i, back = zero, zero, zero
    beta = zero

    def imag_of(row):
        return pltpu.roll(row, 128 - 8, 1)

    for step in range(KRYLOV + 1):
        if step < KRYLOV:
            if step > 0:
                def local(chunk, carry, step=step):
                    _, hr, hi = local_part(step, chunk)
                    hbuf[chunk, 0] = hr
                    hbuf[chunk, 1] = hi
                    return carry

                lax.fori_loop(0, CHUNKS, local, 0)

            def forward(chunk, carry, step=step):
                for copy in direct(step, chunk):
                    copy.wait_recv()
                for copy in relay(step, chunk):
                    copy.start()
                hbuf[chunk] = hbuf[chunk] - (
                    field[15] * big[DIR_Y, step, chunk] + field[17] * big[DIR_X, step, chunk])
                return carry

            lax.fori_loop(0, CHUNKS, forward, 0)
        row = take_sums(step)
        row_i = imag_of(row)
        square = pick(row, 32)
        if step == 0:
            norm = jnp.sqrt(square)
            shift_r = pick(row, 0) / square
            shift_i = pick(row, 8) / square
            beta = norm
            gs = []
        else:
            gs = [(pick(row, k), pick(row, 8 + k)) for k in range(step)]
            used = square
            for gr, gi in gs:
                used = used - (gr * gr + gi * gi)
            norm = jnp.sqrt(used)
            at = sub == step - 1
            col_r = jnp.where(lane < step, row, 0.0) + jnp.where(lane == step - 1, shift_r, 0.0)
            col_i = jnp.where(lane < step, row_i, 0.0) + jnp.where(lane == step - 1, shift_i, 0.0)
            if step > 1:
                col_r = col_r + jnp.where(lane == step - 2, back, 0.0)
            if step < KRYLOV:
                col_r = col_r + jnp.where(lane == step, norm, 0.0)
            hess_r = jnp.where(at, col_r, hess_r)
            hess_i = jnp.where(at, col_i, hess_i)
            pr = pltpu.roll(row, 128 - 16, 1)
            proj_r = jnp.where(at & (lane < step), pr, proj_r)
            proj_i = jnp.where(at & (lane < step), imag_of(pr), proj_i)
            shift_r = shift_r + gs[-1][0]
            shift_i = shift_i + gs[-1][1]
            back = norm
        if step == KRYLOV:
            break
        inv = 1.0 / norm
        br, bi = jnp.where(lane[:1] == step, 1.0, 0.0), jnp.zeros((1, 128), f32)
        for k, (gr, gi) in enumerate(gs):
            tr, ti = cmul(gr[:1], gi[:1], basis_r[k : k + 1], basis_i[k : k + 1])
            br, bi = br - tr, bi - ti
        basis_r = jnp.where(sub == step, wide(br * inv[:1]), basis_r)
        basis_i = jnp.where(sub == step, wide(bi * inv[:1]), basis_i)

        acc[...] = jnp.zeros((40, 8, 128), f32)

        def advance(chunk, carry, step=step, gs=gs, inv=inv, shift_r=shift_r, shift_i=shift_i, back=back):
            for copy in relay(step, chunk):
                copy.wait_recv()
            h = hbuf[chunk] - (field[16] * big[REL_Y, step, chunk] + field[18] * big[REL_X, step, chunk])
            v = big[OWN, step, chunk]
            vr, vi, zr, zi = v[0], v[1], h[0], h[1]
            for k, (gr, gi) in enumerate(gs):
                pv, pz = vbuf[k, chunk], zbuf[k, chunk]
                tr, ti = cmul(gr, gi, pv[0], pv[1])
                vr, vi = vr - tr, vi - ti
                tr, ti = cmul(gr, gi, pz[0], pz[1])
                zr, zi = zr - tr, zi - ti
            vr, vi, zr, zi = vr * inv, vi * inv, zr * inv, zi * inv
            tr, ti = cmul(shift_r, shift_i, vr, vi)
            ur, ui = zr - tr, zi - ti
            if step > 0:
                pv = vbuf[step - 1, chunk]
                ur, ui = ur - back * pv[0], ui - back * pv[1]
            if step + 1 < KRYLOV:
                vbuf[step, chunk, 0] = vr
                vbuf[step, chunk, 1] = vi
                zbuf[step, chunk, 0] = zr
                zbuf[step, chunk, 1] = zi
                big[OWN, step + 1, chunk, 0] = ur
                big[OWN, step + 1, chunk, 1] = ui
            m = mask_ref[chunk]
            mr, mi = m * vr, m * vi
            for k in range(step + 1):
                if k < step:
                    pv = vbuf[k, chunk]
                    pr, pi = pv[0], pv[1]
                else:
                    pr, pi = vr, vi
                acc[k] += jnp.sum(pr * ur + pi * ui, axis=0)
                acc[8 + k] += jnp.sum(pr * ui - pi * ur, axis=0)
                acc[16 + k] += jnp.sum(pr * mr + pi * mi, axis=0)
                acc[24 + k] += jnp.sum(pr * mi - pi * mr, axis=0)
            acc[32] += jnp.sum(ur * ur + ui * ui, axis=0)
            if step + 1 < KRYLOV:
                @pl.when((chunk >= 1) & (chunk <= EARLY))
                def _():
                    for copy in direct(step + 1, chunk - 1):
                        copy.start()
            return carry

        lax.fori_loop(0, CHUNKS, advance, 0)
        post_sums(step + 1)
        if step + 1 < KRYLOV:
            def send_rest(chunk, carry, step=step):
                for copy in direct(step + 1, chunk):
                    copy.start()
                return carry

            lax.fori_loop(EARLY, CHUNKS, send_rest, 0)

    scale = TIME_STEP / 256.0
    ar, ai = scale * hess_i, -scale * hess_r
    eye = jnp.where(sub == lane, 1.0, 0.0)
    er, ei = eye, zero
    for degree in range(10, 0, -1):
        tr, ti = matmul8(ar, ai, er, ei)
        er, ei = eye + tr * (1.0 / degree), ti * (1.0 / degree)
    for _ in range(8):
        er, ei = matmul8(er, ei, er, ei)
    first_r, first_i = wide(er[:1]) * beta, wide(ei[:1]) * beta
    along_r = wide(jnp.sum(jnp.where(sub == lane, first_r, 0.0), axis=1, keepdims=True))
    along_i = wide(jnp.sum(jnp.where(sub == lane, first_i, 0.0), axis=1, keepdims=True))
    pair_r, pair_i = cmul(first_r, -first_i, along_r, along_i)
    weight = jnp.where(lane < sub, 2.0, 1.0)
    weighed = jnp.where(lane < KRYLOV, weight * (pair_r * proj_r - pair_i * proj_i), 0.0)
    held = wide(jnp.sum(jnp.sum(weighed, axis=1, keepdims=True), axis=0, keepdims=True))
    jumps = jnp.full((8, 128), channel, jnp.int32)
    held = jnp.where(jumps < SPINS, held, 524288.0)
    factor = jnp.sqrt(524288.0 / held)
    tr, ti = cmul(along_r, along_i, basis_r, basis_i)
    sent_r = wide(jnp.sum(tr, axis=0, keepdims=True)) * factor
    sent_i = wide(jnp.sum(ti, axis=0, keepdims=True)) * factor
    ds = [(pick(sent_r, k), pick(sent_i, k)) for k in range(KRYLOV)]

    source = jnp.where(channel == 15, DIR_Y, OWN)
    source = jnp.where(channel == 17, DIR_X, source)
    source = jnp.where(channel == 16, REL_Y, source)
    source = jnp.where(channel == 18, REL_X, source)

    def combine(chunk, carry):
        tot_r, tot_i = None, None
        for k, (dr, di) in enumerate(ds):
            v = big[source, k, chunk]
            tr, ti = cmul(dr, di, v[0], v[1])
            tot_r = tr if tot_r is None else tot_r + tr
            tot_i = ti if tot_i is None else tot_i + ti
        prop[0, chunk] = tot_r
        prop[1, chunk] = tot_i
        return carry

    lax.fori_loop(0, CHUNKS, combine, 0)
    delta = jnp.where((channel >= 10) & (channel < 15), jnp.left_shift(1, jnp.clip(channel - 10, 0, 4)), 0)

    def jump(chunk, carry):
        for t in range(PER):
            at = jnp.minimum(chunk * PER + t + delta, TILES - 1)
            vacant = 1.0 - mask_ref[chunk, t]
            for part in range(2):
                v = prop[part, at // PER, at % PER]
                moved = v
                for b in range(7):
                    moved = jnp.where(jumps == b, pltpu.roll(v, 128 - (1 << b), 1), moved)
                for b in range(3):
                    moved = jnp.where(jumps == 7 + b, pltpu.roll(v, 8 - (1 << b), 0), moved)
                out_ref[part, chunk * PER + t] = moved * vacant
        return carry

    lax.fori_loop(0, CHUNKS, jump, 0)

    for number in range(KRYLOV + 1):
        pltpu.make_async_copy(gather.at[number], gather.at[number], red_send.at[number]).wait()
    for kind in range(4):
        for step in range(KRYLOV):
            pltpu.make_async_copy(big.at[OWN, step], big.at[OWN, step], send_sem.at[kind, step]).wait()


def body(amplitudes, couplings, fields, decays, channel):
    shape = (2, TILES, 8, 128)
    vmem = pl.BlockSpec(memory_space=pltpu.VMEM)
    smem = pl.BlockSpec(memory_space=pltpu.SMEM)
    chunk = (2, PER, 8, 128)
    out = pl.pallas_call(
        kernel,
        out_shape=jax.ShapeDtypeStruct(shape, f32),
        in_specs=[vmem, smem, smem, smem, smem],
        out_specs=vmem,
        scratch_shapes=[
            pltpu.VMEM((5, KRYLOV, CHUNKS, *chunk), f32),
            pltpu.VMEM((KRYLOV, CHUNKS, *chunk), f32),
            pltpu.VMEM((KRYLOV, CHUNKS, *chunk), f32),
            pltpu.VMEM((CHUNKS, *chunk), f32),
            pltpu.VMEM((CHUNKS, PER, 8, 128), f32),
            pltpu.VMEM((CHUNKS, PER, 8, 128), f32),
            pltpu.VMEM((CHUNKS, PER, 8, 128), f32),
            pltpu.VMEM((128, 128), f32),
            pltpu.VMEM((40, 8, 128), f32),
            pltpu.VMEM((KRYLOV + 1, 1, 128), f32),
            pltpu.VMEM((KRYLOV + 1, 15, 1, 128), f32),
            pltpu.VMEM((2, CHUNKS, PER, 8, 128), f32),
            pltpu.SemaphoreType.DMA((4, KRYLOV, CHUNKS)),
            pltpu.SemaphoreType.DMA((4, KRYLOV)),
            pltpu.SemaphoreType.DMA((KRYLOV + 1,)),
            pltpu.SemaphoreType.DMA((KRYLOV + 1,)),
        ],
        compiler_params=pltpu.CompilerParams(collective_id=0, has_side_effects=True),
    )(amplitudes.reshape(shape), couplings, fields, decays, channel)
    return out.reshape(amplitudes.shape)


def solution(mesh):
    placed = (P("traj", None, "amp"), P(), P(), P(), P("traj"))
    return jax.shard_map(
        body, mesh=mesh, in_specs=placed, out_specs=P("traj", None, "amp"), check_vma=False
    )
```

```python
import functools

import jax
import jax.numpy as jnp
from jax import lax
from jax.experimental import pallas as pl
from jax.experimental.pallas import tpu as pltpu
from jax.sharding import PartitionSpec as P

SPINS = 19
KRYLOV = 8
TILES = 32
CHUNKS = 16
PER = TILES // CHUNKS
CHUNK_BITS = CHUNKS.bit_length() - 1
LEAD = 8
TOTAL = KRYLOV * CHUNKS
TIME_STEP = 0.7
MESH = pl.DeviceIdType.MESH
OWN, DIR_Y, DIR_X, REL_Y, REL_X = range(5)
highest = lax.Precision.HIGHEST
f32 = jnp.float32


def flip(index, bit):
    step = 1 << bit
    return index + step - 2 * step * ((index // step) % 2)


def flip_by(index, mask):
    for bit in range(4):
        if mask >> bit & 1:
            index = flip(index, bit)
    return index


def wide(value):
    return jnp.broadcast_to(value, (8, 128))


def cmul(ar, ai, br, bi):
    return ar * br - ai * bi, ar * bi + ai * br


class Algebra:
    def __init__(self, sqrt, maximum, minimum):
        self.sqrt, self.maximum, self.minimum = sqrt, maximum, minimum
        self.r, self.ri, self.h, self.t, self.s, self.si = [], [], [], [], [], []

    @staticmethod
    def mul(a, b):
        if a[1] is None and b[1] is None:
            return a[0] * b[0], None
        if a[1] is None:
            return a[0] * b[0], a[0] * b[1]
        if b[1] is None:
            return a[0] * b[0], a[1] * b[0]
        return a[0] * b[0] - a[1] * b[1], a[0] * b[1] + a[1] * b[0]

    @staticmethod
    def join(a, b, sign):
        real = a[0] + b[0] if sign > 0 else a[0] - b[0]
        if b[1] is None:
            return real, a[1]
        if a[1] is None:
            return real, b[1] if sign > 0 else -b[1]
        return real, a[1] + b[1] if sign > 0 else a[1] - b[1]

    def dot(self, pairs, start=None, sign=1):
        total = start
        for a, b in pairs:
            term = self.mul(a, b)
            if total is None:
                total = term if sign > 0 else (-term[0], None if term[1] is None else -term[1])
            else:
                total = self.join(total, term, sign)
        return total

    def absorb(self, m, products, square, last=False):
        conj = lambda a: (a[0], None if a[1] is None else -a[1])
        r = [self.dot([(conj(self.ri[k][l]), products[l]) for l in range(k + 1)]) for k in range(m)]
        if not last:
            used = square
            for a in r:
                used = used - (a[0] * a[0] + a[1] * a[1])
            norm = self.sqrt(self.maximum(used, 1e-10 * square))
            inv = (1.0 / norm, None)
            ri = [self.mul(self.dot([(self.ri[k][l], r[k]) for k in range(l, m)], sign=-1), inv) for l in range(m)]
            self.ri.append(ri + [inv])
            self.r.append(r + [(norm, None)])
        else:
            self.r.append(r)
        if m > 0:
            c = m - 1
            col = self.t[c] + [(self.si[c], None)]
            rows = m if last else m + 1
            out = []
            for l in range(rows):
                a = self.dot([(col[k], self.r[k][l]) for k in range(l, m + 1)])
                a = self.dot([(self.r[c][k], self.h[k][l]) for k in range(max(l - 1, 0), c)], a, -1)
                out.append(self.mul(a, self.ri[c][c]))
            self.h.append(out)

    def start(self, shift, spread):
        root = self.sqrt(spread)
        s0 = 1.0 / root
        self.t.append([shift])
        self.s.append(s0)
        self.si.append(root)
        self.t.append([(spread * s0, None), shift])
        self.s.append(s0 * 0.70710678)
        self.si.append(root * 1.41421356)

    def predict(self, j):
        m = j - 1
        last = self.h[m - 1][m][0]
        last2 = last * last
        if m >= 2:
            before = self.h[m - 2][m - 1][0]
            rise = self.maximum(-0.5 * last2, self.minimum(last2, last2 - before * before))
            next2 = last2 + rise
        else:
            next2 = last2 * 1.5
        nxt = self.sqrt(next2)
        after = self.sqrt(self.maximum(2.0 * next2 - last2, 0.5 * next2))
        shift = self.h[m - 1][m - 1]
        guess = {m - 1: (last, None), m: shift}
        rows = []
        for l in range(m + 1):
            a = self.dot([(self.r[m][k], self.h[k][l]) for k in range(max(l - 1, 0), m)])
            if l in guess:
                a = self.dot([(self.r[m][m], guess[l])], a)
            a = self.dot([(self.t[m][k], self.r[k][l]) for k in range(l, m + 1)], a, -1)
            rows.append(self.mul(a, (self.s[m], None)))
        top = self.mul(self.r[m][m], (nxt * self.s[m], None))
        image = []
        for l in range(m + 1):
            a = self.dot([(rows[k], self.h[k][l]) for k in range(max(l - 1, 0), m)])
            if l in guess:
                a = self.dot([(rows[m], guess[l])], a)
            if l == m:
                a = self.dot([(top, (nxt, None))], a)
            image.append(a)
        lead = self.dot([(rows[m], (nxt, None)), (top, shift)])
        lead = self.mul(lead, (1.0 / top[0], None))
        rest = [self.join(image[l], self.mul(lead, rows[l]), -1) for l in range(m + 1)]
        t = [self.dot([(self.ri[k][l], rest[k]) for k in range(l, m + 1)]) for l in range(m + 1)]
        self.t.append(t + [lead])
        self.s.append(1.0 / after)
        self.si.append(after)


def matmul8(ar, ai, br, bi):
    out_r, out_i = None, None
    for k in range(KRYLOV):
        cr, ci = ar[:, k : k + 1], ai[:, k : k + 1]
        rr, ri = br[k : k + 1, :], bi[k : k + 1, :]
        tr, ti = cr * rr - ci * ri, cr * ri + ci * rr
        out_r = tr if out_r is None else out_r + tr
        out_i = ti if out_i is None else out_i + ti
    return out_r, out_i


def kernel(
    amp_ref, coup, field, decay, chan, out_ref,
    big, hbuf, diag_r, diag_i, mask_ref, lanes_ref, acc, total_ref, gather, prop,
    recv_sem, send_sem, red_recv, red_send,
):
    me = lax.axis_index("amp")
    y, x = me % 4, me // 4
    near_y, near_x = x * 4 + flip(y, 0), flip(x, 0) * 4 + y
    far_y, far_x = x * 4 + 3 - y, (3 - x) * 4 + y

    barrier = pltpu.get_barrier_semaphore()
    for mask in range(1, 16):
        pl.semaphore_signal(barrier, inc=1, device_id={"amp": flip_by(me, mask)}, device_id_type=MESH)

    lane = lax.broadcasted_iota(jnp.int32, (8, 128), 1)
    sub = lax.broadcasted_iota(jnp.int32, (8, 128), 0)
    low = sub * 128 + lane

    def copies(table, at):
        return [
            pltpu.make_async_remote_copy(
                src_ref=big.at[source, at], dst_ref=big.at[kind, at],
                send_sem=send_sem.at[kind - 1], recv_sem=recv_sem.at[kind - 1, at],
                device_id={"amp": target}, device_id_type=MESH)
            for kind, source, target in table
        ]

    def direct(at):
        return copies(((DIR_Y, OWN, near_y), (DIR_X, OWN, near_x)), at)

    def relay(at):
        return copies(((REL_Y, DIR_Y, far_y), (REL_X, DIR_X, far_x)), at)

    def sum_copy(number, mask):
        return pltpu.make_async_remote_copy(
            src_ref=total_ref.at[number], dst_ref=gather.at[number, mask - 1],
            send_sem=red_send.at[number], recv_sem=red_recv.at[number],
            device_id={"amp": flip_by(me, mask)}, device_id_type=MESH)

    def post_sums(number):
        rows = lax.broadcasted_iota(jnp.int32, (40, 128), 0)
        cols = lax.broadcasted_iota(jnp.int32, (40, 128), 1)
        by_lane = jnp.sum(acc[...], axis=1)
        by_row = jnp.sum(by_lane, axis=1, keepdims=True)
        total_ref[number] = jnp.sum(jnp.where(rows == cols, by_row, 0.0), axis=0, keepdims=True)
        for mask in range(1, 16):
            sum_copy(number, mask).start()

    def take_sums(number):
        pltpu.make_async_copy(gather.at[number], gather.at[number], red_recv.at[number]).wait()
        terms = [total_ref[number]] + [gather[number, i] for i in range(15)]
        while len(terms) > 1:
            terms = [terms[i] + terms[i + 1] for i in range(0, len(terms), 2)]
        return wide(terms[0])

    def pick(row, at):
        return wide(jnp.sum(jnp.where(lane == at, row, 0.0), axis=1, keepdims=True))

    def forward(at):
        for copy in direct(at):
            copy.wait_recv()
        for copy in relay(at):
            copy.start()

    for tile in range(TILES):
        for part in range(2):
            big[OWN, tile // PER, part, tile % PER] = amp_ref[tile * 8 : tile * 8 + 8, part]
    pl.semaphore_wait(barrier, 15)

    def send_first(at, carry):
        for copy in direct(at):
            copy.start()
        return carry

    lax.fori_loop(0, CHUNKS, send_first, 0)

    z = [1.0 - 2.0 * (low >> i & 1).astype(f32) for i in range(10)]
    base_r = jnp.zeros((8, 128), f32)
    base_i = jnp.zeros((8, 128), f32)
    for i in range(9):
        base_r = base_r - coup[i] * (z[i] * z[i + 1])
    for i in range(10):
        base_i = base_i - (0.25 * decay[i]) * (1.0 - z[i])
    zdev = [(1 - 2 * ((me // (1 << b)) % 2)).astype(f32) for b in range(4)]
    dev_r = -(coup[15] * zdev[0] * zdev[1] + coup[16] * zdev[1] * zdev[2] + coup[17] * zdev[2] * zdev[3])
    dev_i = jnp.float32(0.0)
    for b in range(4):
        dev_i = dev_i - 0.25 * decay[15 + b] * (1.0 - zdev[b])
    bond = coup[9] * z[9]
    channel = chan[0]
    shifts = jnp.full((8, 128), channel, jnp.int32)
    for tile in range(TILES):
        zt = [1.0 - 2.0 * (tile >> b & 1) for b in range(5)]
        sr, si = dev_r - coup[14] * zdev[0] * zt[4], dev_i
        for b in range(4):
            sr = sr - coup[10 + b] * (zt[b] * zt[b + 1])
        for b in range(5):
            if tile >> b & 1:
                si = si - 0.5 * decay[10 + b]
        diag_r[tile // PER, tile % PER] = (base_r - bond * zt[0]) + sr
        diag_i[tile // PER, tile % PER] = base_i + si
        spot = low + (tile * 1024 + me * 32768)
        mask_ref[tile // PER, tile % PER] = (spot >> shifts & 1).astype(f32)
    li = lax.broadcasted_iota(jnp.int32, (128, 128), 0)
    lj = lax.broadcasted_iota(jnp.int32, (128, 128), 1)
    table = jnp.zeros((128, 128), f32)
    for i in range(7):
        table = table + jnp.where((li ^ lj) == 1 << i, field[i], 0.0)
    lanes_ref[...] = table
    acc[...] = jnp.zeros((40, 8, 128), f32)

    def local_part(step, chunk):
        base = step * CHUNKS
        v = big[OWN, base + chunk]
        flips = lax.dot_general(
            v.reshape(2 * PER * 8, 128), lanes_ref[...], (((1,), (0,)), ((), ())),
            precision=highest, preferred_element_type=f32).reshape(2 * PER, 8, 128)
        w = v.reshape(2 * PER, 8, 128)
        s3 = lax.broadcasted_iota(jnp.int32, (2 * PER, 8, 128), 1)
        for b in range(2):
            rows = 1 << b
            up = pltpu.roll(w, 8 - rows, 1)
            down = pltpu.roll(w, rows, 1)
            flips = flips + field[7 + b] * jnp.where((s3 >> b & 1) == 0, up, down)
        flips = flips + field[9] * pltpu.roll(w, 4, 1)
        flips = flips.reshape(2, PER, 8, 128)
        for b in range(5 - CHUNK_BITS):
            order = [t ^ (1 << b) for t in range(PER)]
            flips = flips + field[10 + b] * jnp.concatenate([v[:, t : t + 1] for t in order], axis=1)
        for b in range(CHUNK_BITS):
            flips = flips + field[15 - CHUNK_BITS + b] * big[OWN, base + flip(chunk, b)]
        dr, di = diag_r[chunk], diag_i[chunk]
        hr = dr * v[0] - di * v[1] - flips[0]
        hi = dr * v[1] + di * v[0] - flips[1]
        return v, hr, hi

    def first(chunk, carry):
        v, hr, hi = local_part(0, chunk)
        hbuf[chunk, 0] = hr
        hbuf[chunk, 1] = hi
        acc[0] += jnp.sum(v[0] * hr + v[1] * hi, axis=0)
        acc[8] += jnp.sum(v[0] * hi - v[1] * hr, axis=0)
        acc[16] += jnp.sum(hr * hr + hi * hi, axis=0)
        acc[32] += jnp.sum(v[0] * v[0] + v[1] * v[1], axis=0)
        return carry

    lax.fori_loop(0, CHUNKS, first, 0)
    post_sums(0)

    def lead_in(at, carry):
        forward(at)
        return carry

    lax.fori_loop(0, LEAD, lead_in, 0)

    algebra = Algebra(jnp.sqrt, jnp.maximum, jnp.minimum)
    row = take_sums(0)
    square = pick(row, 32)
    algebra.absorb(0, [], square)
    beta = jnp.sqrt(square)
    shift = (pick(row, 0) / square, pick(row, 8) / square)
    spread = pick(row, 16) / square - (shift[0] * shift[0] + shift[1] * shift[1])
    for b in range(15, 19):
        spread = spread + field[b] * field[b]
    algebra.start(shift, spread)

    zero = jnp.zeros((8, 128), f32)
    proj_r, proj_i = zero, zero
    hess_r, hess_i = zero, zero

    def absorb(number):
        nonlocal proj_r, proj_i, hess_r, hess_i
        row = take_sums(number)
        products = [(pick(row, k), pick(row, 8 + k)) for k in range(min(number, KRYLOV))]
        algebra.absorb(number, products, pick(row, 32), last=number == KRYLOV)
        here = (sub == number - 1) & (lane < number)
        proj_r = jnp.where(here, pltpu.roll(row, 128 - 16, 1), proj_r)
        proj_i = jnp.where(here, pltpu.roll(row, 128 - 24, 1), proj_i)
        for l, value in enumerate(algebra.h[number - 1]):
            spot = (sub == number - 1) & (lane == l)
            hess_r = jnp.where(spot, value[0], hess_r)
            if value[1] is not None:
                hess_i = jnp.where(spot, value[1], hess_i)

    for step in range(KRYLOV):
        if step >= 2:
            absorb(step - 1)
            algebra.predict(step)
        ts, scale = algebra.t[step], algebra.s[step]
        acc[...] = jnp.zeros((40, 8, 128), f32)

        def advance(chunk, carry, step=step, ts=ts, scale=scale):
            at = step * CHUNKS + chunk
            if step + 1 < KRYLOV:
                forward(at + LEAD)
            else:
                @pl.when(chunk < CHUNKS - LEAD)
                def _():
                    forward(at + LEAD)
            if step == 0:
                h = hbuf[chunk]
            else:
                _, hr, hi = local_part(step, chunk)
                h = jnp.stack([hr, hi])
            h = h - (field[15] * big[DIR_Y, at] + field[17] * big[DIR_X, at])
            ur, ui = h[0], h[1]
            for k, t in enumerate(ts):
                p = big[OWN, k * CHUNKS + chunk]
                if t[1] is None:
                    ur, ui = ur - t[0] * p[0], ui - t[0] * p[1]
                else:
                    tr, ti = cmul(t[0], t[1], p[0], p[1])
                    ur, ui = ur - tr, ui - ti
            for copy in relay(at):
                copy.wait_recv()
            h = field[16] * big[REL_Y, at] + field[18] * big[REL_X, at]
            ur, ui = (ur - h[0]) * scale, (ui - h[1]) * scale
            if step + 1 < KRYLOV:
                big[OWN, at + CHUNKS, 0] = ur
                big[OWN, at + CHUNKS, 1] = ui
            m = mask_ref[chunk]
            v = big[OWN, at]
            mr, mi = m * v[0], m * v[1]
            for k in range(step + 1):
                p = big[OWN, k * CHUNKS + chunk]
                pr, pi = p[0], p[1]
                acc[k] += jnp.sum(pr * ur + pi * ui, axis=0)
                acc[8 + k] += jnp.sum(pr * ui - pi * ur, axis=0)
                acc[16 + k] += jnp.sum(pr * mr + pi * mi, axis=0)
                acc[24 + k] += jnp.sum(pr * mi - pi * mr, axis=0)
            acc[32] += jnp.sum(ur * ur + ui * ui, axis=0)
            if step + 1 < KRYLOV:
                for copy in direct(at + CHUNKS):
                    copy.start()
            return carry

        lax.fori_loop(0, CHUNKS, advance, 0)
        post_sums(step + 1)

    absorb(KRYLOV - 1)
    absorb(KRYLOV)

    size = TIME_STEP / 256.0
    ar, ai = size * hess_i, -size * hess_r
    eye = jnp.where(sub == lane, 1.0, 0.0)
    er, ei = eye, zero
    for degree in range(10, 0, -1):
        tr, ti = matmul8(ar, ai, er, ei)
        er, ei = eye + tr * (1.0 / degree), ti * (1.0 / degree)
    for _ in range(8):
        er, ei = matmul8(er, ei, er, ei)
    first_r, first_i = wide(er[:1]) * beta, wide(ei[:1]) * beta
    weights = [(pick(first_r, k), pick(first_i, k)) for k in range(KRYLOV)]
    ds = [algebra.dot([(algebra.ri[k][l], weights[k]) for k in range(l, KRYLOV)]) for l in range(KRYLOV)]
    across_r, across_i, along_r, along_i = zero, zero, zero, zero
    for k, (dr, di) in enumerate(ds):
        across_r, across_i = jnp.where(lane == k, dr, across_r), jnp.where(lane == k, di, across_i)
        along_r, along_i = jnp.where(sub == k, dr, along_r), jnp.where(sub == k, di, along_i)
    pair_r, pair_i = cmul(across_r, -across_i, along_r, along_i)
    weighed = jnp.where(lane < sub, 2.0, 1.0) * (pair_r * proj_r - pair_i * proj_i)
    held = wide(jnp.sum(jnp.sum(weighed, axis=1, keepdims=True), axis=0, keepdims=True))
    held = jnp.where(shifts < SPINS, held, 524288.0)
    factor = jnp.sqrt(524288.0 / held)
    ds = [(dr * factor, di * factor) for dr, di in ds]

    source = jnp.where(channel == 15, DIR_Y, OWN)
    source = jnp.where(channel == 17, DIR_X, source)
    source = jnp.where(channel == 16, REL_Y, source)
    source = jnp.where(channel == 18, REL_X, source)

    def combine(chunk, carry):
        tot_r, tot_i = None, None
        for k, (dr, di) in enumerate(ds):
            v = big[source, k * CHUNKS + chunk]
            tr, ti = cmul(dr, di, v[0], v[1])
            tot_r = tr if tot_r is None else tot_r + tr
            tot_i = ti if tot_i is None else tot_i + ti
        prop[0, chunk] = tot_r
        prop[1, chunk] = tot_i
        return carry

    lax.fori_loop(0, CHUNKS, combine, 0)
    delta = jnp.where((channel >= 10) & (channel < 15), jnp.left_shift(1, jnp.clip(channel - 10, 0, 4)), 0)

    def jump(chunk, carry):
        for t in range(PER):
            at = jnp.minimum(chunk * PER + t + delta, TILES - 1)
            vacant = 1.0 - mask_ref[chunk, t]
            for part in range(2):
                v = prop[part, at // PER, at % PER]
                moved = v
                for b in range(7):
                    moved = jnp.where(shifts == b, pltpu.roll(v, 128 - (1 << b), 1), moved)
                for b in range(3):
                    moved = jnp.where(shifts == 7 + b, pltpu.roll(v, 8 - (1 << b), 0), moved)
                out_ref[pl.ds((chunk * PER + t) * 8, 8), part] = moved * vacant
        return carry

    lax.fori_loop(0, CHUNKS, jump, 0)

    for number in range(KRYLOV + 1):
        pltpu.make_async_copy(gather.at[number], gather.at[number], red_send.at[number]).wait()
    for kind in range(4):
        pltpu.make_async_copy(big.at[OWN], big.at[OWN], send_sem.at[kind]).wait()


def body(amplitudes, couplings, fields, decays, channel):
    vmem = pl.BlockSpec(memory_space=pltpu.VMEM)
    smem = pl.BlockSpec(memory_space=pltpu.SMEM)
    chunk = (2, PER, 8, 128)
    out = pl.pallas_call(
        kernel,
        out_shape=jax.ShapeDtypeStruct((TILES * 8, 2, 128), f32),
        in_specs=[vmem, smem, smem, smem, smem],
        out_specs=vmem,
        scratch_shapes=[
            pltpu.VMEM((5, TOTAL, *chunk), f32),
            pltpu.VMEM((CHUNKS, *chunk), f32),
            pltpu.VMEM((CHUNKS, PER, 8, 128), f32),
            pltpu.VMEM((CHUNKS, PER, 8, 128), f32),
            pltpu.VMEM((CHUNKS, PER, 8, 128), f32),
            pltpu.VMEM((128, 128), f32),
            pltpu.VMEM((40, 8, 128), f32),
            pltpu.VMEM((KRYLOV + 1, 1, 128), f32),
            pltpu.VMEM((KRYLOV + 1, 15, 1, 128), f32),
            pltpu.VMEM((2, CHUNKS, PER, 8, 128), f32),
            pltpu.SemaphoreType.DMA((4, TOTAL)),
            pltpu.SemaphoreType.DMA((4,)),
            pltpu.SemaphoreType.DMA((KRYLOV + 1,)),
            pltpu.SemaphoreType.DMA((KRYLOV + 1,)),
        ],
        compiler_params=pltpu.CompilerParams(collective_id=0, has_side_effects=True),
    )(amplitudes.reshape(2, TILES * 8, 128).transpose(1, 0, 2), couplings, fields, decays, channel)
    return out.transpose(1, 0, 2).reshape(amplitudes.shape)


def solution(mesh):
    placed = (P("traj", None, "amp"), P(), P(), P(), P("traj"))
    return jax.shard_map(
        body, mesh=mesh, in_specs=placed, out_specs=P("traj", None, "amp"), check_vma=False
    )
```
